128 devices in a mesh: dp: 16 (over y, z), mp: 8 (over x, core).
Axes of the slice: x: 4, y: 4, z: 4, core: 2. Of those that a mesh axis runs over, the one named last changes fastest.
Arguments:
- patch_query: bfloat16 [4096, 4096], P('dp'), may hold values from -6 to 6
- key_cache: bfloat16 [4096, 16, 4096], P('dp', None, 'mp'), may hold values from -48 to 48
- value_cache: bfloat16 [4096, 16, 4096], P('dp', None, 'mp'), may hold values from -6 to 6
- cache_len: int32 [4096], P('dp'), may hold values from 1 to 16
- patch_end: int32 [4096], P('dp'), may hold values from 0 to 1, as said below
- ended_index: int32 [2048], P('dp'), may hold values from 0 to 256, as said below
- pool_out: bfloat16 [4096, 4096], P('mp'), may hold values from -0.09375 to 0.09375
- norm_gain: float32 [2, 4096], replicated, may hold values from 0.1 to 1.9
- w_in: bfloat16 [2, 4096, 2, 14336], P(None, 'dp', None, 'mp'), may hold values from -0.09375 to 0.09375
- w_out: bfloat16 [2, 14336, 4096], P(None, 'mp', 'dp'), may hold values from -0.046875 to 0.046875
Outputs:
- global_out: bfloat16 [4096, 4096], P('dp')
The draws below stay inside these ranges and needn't reach their ends.
Inputs may be any that keep to these rules, and one draw needn't show every extreme that they name: `patch_end`: each index of dp has at most 128 ended patches among its 256 sequences, and some index has exactly 128. `ended_index`: each aligned block of 128 entries lists, in increasing order, the local indices of the ended sequences of that index of dp, then 256 in the remaining entries.
All inputs are finite; a program needn't handle non-finite values.
Results may differ from the reference program's by a relative error of at most 0.024.
Values may be sent and summed in bfloat16 or wider, within the bound.
No kernel may reach another device: no remote copies, remote signals or barrier semaphores. Data moves between devices by JAX's collectives and lax.ppermute only.
A program may use at most 128 MiB of HBM per device.

```python
import jax
import jax.numpy as jnp
from jax import lax

D = 4096
FF = 14336
HEAD_DIM = 128
LAYERS = 2
PATCH = 16
SEQ_DEV = 256
CAP = 128
B = 4096
R = 2048
N_DP = 16
N_MP = 8


def query_and_keys(key):
    query_draw = jnp.clip(jax.random.normal(jax.random.fold_in(key, 11), (B, D), jnp.float32), -6.0, 6.0)
    keys_draw = jnp.clip(jax.random.normal(jax.random.fold_in(key, 12), (B, PATCH, D), jnp.float32), -6.0, 6.0)
    return (query_draw, keys_draw)


def draw_patch_query(key, part):
    return query_and_keys(key)[0].astype(jnp.bfloat16)


def draw_key_cache(key, part):
    return query_and_keys(key)[1].astype(jnp.bfloat16)


def ended_tables(key):
    shards = B // SEQ_DEV
    shard_keys = jax.random.split(jax.random.fold_in(key, 21), shards)
    counts = jax.random.randint(jax.random.fold_in(key, 22), (shards,), CAP // 4, CAP + 1)
    fullest = jax.random.randint(jax.random.fold_in(key, 23), (), 0, shards)
    counts = counts.at[fullest].set(CAP)

    def single_shard(shard_key, ended_count):
        permuted = jax.random.permutation(shard_key, SEQ_DEV)
        ranking = jnp.argsort(permuted, stable=True)
        flagged = (ranking < ended_count).astype(jnp.int32)
        position = jnp.cumsum(flagged) - 1
        target = jnp.where(flagged == 1, position, CAP)
        slot_index = jnp.full((CAP,), SEQ_DEV, jnp.int32).at[target].set(jnp.arange(SEQ_DEV, dtype=jnp.int32), mode='drop')
        return (flagged, slot_index)
    flagged, slot_index = jax.vmap(single_shard)(shard_keys, counts)
    return (flagged.reshape(-1).astype(jnp.int32), slot_index.reshape(-1).astype(jnp.int32))


def draw_patch_end(key, part):
    return ended_tables(key)[0]


def draw_ended_index(key, part):
    return ended_tables(key)[1]


def plant(drawn, rng, smallest, largest):
    index_at = [jax.random.randint(jax.random.fold_in(rng, axis), (), 0, length) for axis, length in enumerate(drawn.shape)]
    longest = drawn.shape.index(max(drawn.shape))
    beside = index_at[:longest] + [(index_at[longest] + 1) % drawn.shape[longest]] + index_at[longest + 1:]
    return drawn.at[tuple(index_at)].set(smallest).at[tuple(beside)].set(largest)


def levels(stream_key, dims, pieces, low, largest):
    factor_of, own = 1.0, jax.random.fold_in(stream_key, 6)
    for dim, parts in pieces:
        draws = jnp.exp(jax.random.uniform(jax.random.fold_in(own, dim), (parts,), jnp.float32, low / len(pieces), largest / len(pieces)))
        factor_of = factor_of * jnp.repeat(draws, dims[dim] // parts).reshape([-1 if axis == dim else 1 for axis in range(len(dims))])
    return factor_of


def gaussian(rng, dims, scale, most, pieces=(), held_as=jnp.bfloat16):
    values = scale * jax.random.normal(rng, dims, jnp.float32)
    if pieces:
        values = values * levels(rng, dims, pieces, -0.22, 0.18)
    return jnp.clip(values, -most, most).astype(held_as)


def setup_inputs(seed: int = 0) -> dict:
    streams_of = jax.random.split(jax.random.key(seed), 11)
    return {
        "patch_query": draw_patch_query(jax.random.fold_in(streams_of[10], 71), 0),
        "key_cache": draw_key_cache(jax.random.fold_in(streams_of[10], 71), 0),
        "value_cache": gaussian(streams_of[2], (B, PATCH, D), 1.0, 6.0, ((0, 16), (2, 8))),
        "cache_len": plant(jax.random.randint(streams_of[3], (B,), 1, PATCH + 1), jax.random.fold_in(streams_of[3], 1), 1, PATCH).astype(jnp.int32),
        "patch_end": draw_patch_end(jax.random.fold_in(streams_of[10], 71), 0),
        "ended_index": draw_ended_index(jax.random.fold_in(streams_of[10], 71), 0),
        "pool_out": gaussian(streams_of[6], (D, D), D ** -0.5, 0.09375, ((0, 8),)),
        "norm_gain": jnp.clip(1.0 + 0.18 * jax.random.normal(streams_of[7], (LAYERS, D), jnp.float32), 0.1, 1.9),
        "w_in": gaussian(streams_of[8], (LAYERS, D, 2, FF), D ** -0.5, 0.09375, ((1, 16), (3, 8))),
        "w_out": gaussian(streams_of[9], (LAYERS, FF, D), FF ** -0.5, 0.046875, ((1, 8), (2, 16))),
    }


norm_floor = 1e-05

def rounded(value):
    return lax.optimization_barrier(value.astype(jnp.bfloat16)).astype(jnp.float32)

def attend_all(query, keys, values, lengths):
    total_rows, patch_len, full_width = keys.shape
    head_count = full_width // HEAD_DIM
    query_heads = query.astype(jnp.float32).reshape(total_rows, head_count, HEAD_DIM)
    key_heads = keys.astype(jnp.float32).reshape(total_rows, patch_len, head_count, HEAD_DIM)
    value_heads = values.astype(jnp.float32).reshape(total_rows, patch_len, head_count, HEAD_DIM)
    scores = jnp.einsum('shd,sphd->shp', query_heads, key_heads, precision=lax.Precision.HIGHEST) * HEAD_DIM ** (-0.5)
    live_mask = jnp.arange(patch_len, dtype=jnp.int32)[None, None, :] < lengths[:, None, None]
    scores = jnp.where(live_mask, scores, jnp.float32(-1e+30))
    top_score = lax.optimization_barrier(jnp.max(scores, axis=2, keepdims=True))
    expo = jnp.where(live_mask, jnp.exp(scores - top_score), jnp.float32(0.0))
    weights = (expo / lax.optimization_barrier(jnp.sum(expo, axis=2, keepdims=True))).astype(jnp.bfloat16)
    mixed = jnp.einsum('shp,sphd->shd', weights.astype(jnp.float32), value_heads, precision=lax.Precision.HIGHEST)
    return mixed.astype(jnp.bfloat16).reshape(total_rows, full_width)

def blocked_product(left, right, blocks):
    rows = left.shape[0]
    inner = left.shape[1] // blocks
    left_blocks = left.reshape(rows, blocks, inner)
    right_blocks = right.reshape(blocks, inner, right.shape[1])

    def add_block(index, carry):
        left_part = lax.dynamic_index_in_dim(left_blocks, index, 1, keepdims=False).astype(jnp.float32)
        right_part = lax.dynamic_index_in_dim(right_blocks, index, 0, keepdims=False).astype(jnp.float32)
        term = jnp.dot(left_part, right_part, precision=lax.Precision.HIGHEST, preferred_element_type=jnp.float32)
        return carry + rounded(term)
    start_value = jnp.zeros((rows, right.shape[1]), jnp.float32)
    return lax.fori_loop(0, blocks, add_block, start_value)

def reference(patch_query, key_cache, value_cache, cache_len, patch_end, ended_index, pool_out, norm_gain, w_in, w_out):
    attended = attend_all(patch_query, key_cache, value_cache, cache_len)
    pooled = patch_query.astype(jnp.float32) + blocked_product(attended, pool_out, N_MP)
    owner = jnp.arange(R, dtype=jnp.int32) // CAP
    valid = ended_index < SEQ_DEV
    rows = (owner * SEQ_DEV + jnp.minimum(ended_index, SEQ_DEV - 1)).astype(jnp.int32)
    state = jnp.where(valid[:, None], pooled[rows], jnp.float32(0.0))
    for layer_idx in range(LAYERS):
        mean_square = lax.optimization_barrier(jnp.mean(state * state, axis=1, keepdims=True))
        normed = (state * lax.rsqrt(mean_square + norm_floor) * norm_gain[layer_idx][None, :]).astype(jnp.bfloat16)
        gate_up = blocked_product(normed, w_in[layer_idx].reshape(D, 2 * FF), N_DP)
        hidden = (jax.nn.silu(gate_up[:, :FF]) * gate_up[:, FF:]).astype(jnp.bfloat16)
        ffn = blocked_product(hidden, w_out[layer_idx], N_MP).astype(jnp.bfloat16)
        state = state + ffn.astype(jnp.float32)
    placed = jnp.zeros((B, D), jnp.float32).at[rows].add(jnp.where(valid[:, None], state, jnp.float32(0.0)))
    return (placed * patch_end.astype(jnp.float32)[:, None]).astype(jnp.bfloat16)
```

```python
import jax
import jax.numpy as jnp
from jax import lax
from jax.sharding import Mesh, PartitionSpec as P

HEAD_DIM = 128
NORM_FLOOR = 1e-05
BF16 = jnp.bfloat16
F32 = jnp.float32


def fetch(value, axis, offset):
    size = lax.axis_size(axis)
    return lax.ppermute(value, axis, [(j, (j - offset) % size) for j in range(size)])


def rotated(value, start, axis):
    twice = jnp.concatenate([value, value], axis=axis)
    return lax.dynamic_slice_in_dim(twice, start, value.shape[axis], axis)


def attend_local(query_cols, keys, values, lengths):
    seq_rows, patch_len, heads_width = keys.shape
    head_count = heads_width // HEAD_DIM
    query_heads = query_cols.reshape(seq_rows, head_count, HEAD_DIM)
    key_heads = keys.reshape(seq_rows, patch_len, head_count, HEAD_DIM)
    value_heads = values.reshape(seq_rows, patch_len, head_count, HEAD_DIM)
    scores = jnp.einsum(
        "shd,sphd->shp", query_heads, key_heads, preferred_element_type=F32
    ) * HEAD_DIM ** (-0.5)
    live_mask = jnp.arange(patch_len, dtype=jnp.int32)[None, None, :] < lengths[:, None, None]
    scores = jnp.where(live_mask, scores, F32(-1e30))
    top_score = jnp.max(scores, axis=2, keepdims=True)
    expo = jnp.where(live_mask, jnp.exp(scores - top_score), F32(0.0))
    weights = (expo / jnp.sum(expo, axis=2, keepdims=True)).astype(BF16)
    mixed = jnp.einsum("shp,sphd->shd", weights, value_heads, preferred_element_type=F32)
    return mixed.astype(BF16).reshape(seq_rows, heads_width)


def gather_weight(block):
    half = block.shape[0] // 2
    up = fetch(block, "z", 1)
    down = fetch(block, "z", 3)
    far = jnp.concatenate([fetch(up[:half], "z", 1), fetch(down[half:], "z", 3)])
    return block, up, far, down


def gather_y(value):
    far = fetch(value, "y", 2)
    return value, fetch(value, "y", 1), far, fetch(value, "y", 3)


def reduce_mp(partial):
    pair = partial[:, 0].astype(F32) + fetch(partial[:, 1], "c", 1).astype(F32)
    pair_half = pair.astype(BF16)
    total = pair[:, 0]
    for step in (2, 1, 3):
        total = total + fetch(pair_half[:, (-step) % 4], "x", step).astype(F32)
    return total


def gather_mp(piece):
    own_core = jnp.stack([piece, fetch(piece, "x", 1), fetch(piece, "x", 2), fetch(piece, "x", 3)], axis=1)
    return jnp.stack([own_core, fetch(own_core, "c", 1)], axis=1)


def per_device(
    patch_query,
    key_cache,
    value_cache,
    cache_len,
    patch_end,
    ended_index,
    pool_out,
    norm_gain,
    w_in,
    w_out,
):
    seq_rows, width = patch_query.shape
    heads_width = key_cache.shape[2]
    layers, block_cols, _, hidden_local = w_in.shape
    y = lax.axis_index("y")
    z = lax.axis_index("z")
    x = lax.axis_index("x")
    c = lax.axis_index("c")
    quarter = width // 4

    ins, outs = [], []
    for layer_idx in range(layers):
        ins.append(gather_weight(w_in[layer_idx].reshape(block_cols, 2 * hidden_local)))
        outs.append(gather_weight(w_out[layer_idx].T))

    def my_cols(value):
        part = lax.dynamic_slice_in_dim(value, y * quarter, quarter, value.ndim - 1)
        blocks = part.reshape(*part.shape[:-1], 4, block_cols)
        return rotated(blocks, z, blocks.ndim - 2).reshape(part.shape)

    slots = ended_index.reshape(2, 4, 16)
    slots = rotated(rotated(slots, c, 0), x, 1)
    slot_of = slots.reshape(-1)
    picker = (slot_of[:, None] == jnp.arange(seq_rows, dtype=jnp.int32)[None, :]).astype(BF16)

    own_query = jnp.dot(picker[:16], patch_query, preferred_element_type=F32).astype(BF16)
    query_blocks = rotated(own_query.reshape(16, 4, quarter), y, 1)
    query_rows = jnp.stack(
        [query_blocks[:, 0]] + [fetch(query_blocks[:, (-s) % 4], "y", s) for s in (1, 2, 3)]
    ).reshape(4, 16, 4, block_cols)
    query_rows = rotated(query_rows, z, 2).reshape(4, 16, quarter).astype(F32)

    mp_index = x * 2 + c
    query_cols = lax.dynamic_slice_in_dim(patch_query, mp_index * heads_width, heads_width, 1)
    attended = attend_local(query_cols, key_cache, value_cache, cache_len)
    chosen = jnp.dot(picker, attended, preferred_element_type=F32).astype(BF16)
    all_chosen = jnp.concatenate(gather_y(chosen))
    partial = jnp.dot(all_chosen, my_cols(pool_out), preferred_element_type=F32).astype(BF16)
    state = query_rows + reduce_mp(partial.reshape(4, 2, 4, 16, quarter))

    gains = my_cols(norm_gain)
    for layer_idx in range(layers):
        squares = jnp.sum(state * state, axis=2)
        total = squares
        for step in (2, 1, 3):
            total = total + jnp.roll(fetch(squares, "y", step), step, axis=0)
        scale = lax.rsqrt(total * (1.0 / width) + NORM_FLOOR)
        normed = (state * scale[:, :, None] * gains[layer_idx]).astype(BF16)
        rows = gather_mp(normed).reshape(4, 128, quarter)
        weight_in = jnp.concatenate(ins[layer_idx])
        weight_out = jnp.concatenate(outs[layer_idx])

        def product(step):
            return jnp.dot(rows[step], weight_in, preferred_element_type=F32)

        arrived = [fetch(product((-step) % 4).astype(BF16), "y", step) for step in (2, 1, 3)]
        gate_up = product(0)
        for block in arrived:
            gate_up = gate_up + block.astype(F32)
        hidden = (jax.nn.silu(gate_up[:, :hidden_local]) * gate_up[:, hidden_local:]).astype(BF16)
        all_hidden = jnp.concatenate(gather_y(hidden))
        partial = lax.dot_general(
            all_hidden, weight_out, (((1,), (1,)), ((), ())), preferred_element_type=F32
        ).astype(BF16)
        ffn = reduce_mp(partial.reshape(4, 2, 4, 16, quarter))
        state = state + ffn.astype(BF16).astype(F32)

    piece = state.astype(BF16)
    mine = jnp.stack([piece[0]] + [fetch(piece[(-s) % 4], "y", s) for s in (1, 2, 3)], axis=1)
    mine = rotated(rotated(mine.reshape(16, 4, 4, block_cols), (4 - y) % 4, 1), (4 - z) % 4, 2)
    whole = gather_mp(mine.reshape(1, 16, width)).reshape(128, width)
    placed = lax.dot_general(picker, whole, (((0,), (0,)), ((), ())), preferred_element_type=F32)
    return (placed * patch_end.astype(F32)[:, None]).astype(BF16)


def solution(mesh):
    torus = Mesh(mesh.devices.reshape(4, 4, 4, 2), ("y", "z", "x", "c"))
    dp, mp = ("y", "z"), ("x", "c")
    in_specs = (
        P(dp, None),
        P(dp, None, mp),
        P(dp, None, mp),
        P(dp),
        P(dp),
        P(dp),
        P(mp, None),
        P(),
        P(None, dp, None, mp),
        P(None, mp, dp),
    )
    return jax.shard_map(
        per_device, mesh=torus, in_specs=in_specs, out_specs=P(dp, None), check_vma=False
    )
```

```python
import jax
import jax.numpy as jnp
from jax import lax
from jax.experimental import pallas as pl
from jax.experimental.pallas import tpu as pltpu
from jax.sharding import Mesh, PartitionSpec as P


HEAD_DIM = 128
NORM_FLOOR = 1e-05
BF16 = jnp.bfloat16
F32 = jnp.float32
BLOCK = 256


def fetch(value, axis, offset):
    size = lax.axis_size(axis)
    return lax.ppermute(value, axis, [(j, (j - offset) % size) for j in range(size)])


def fetch_plane(value, offset, core_axis):
    pairs = []
    for y in range(4):
        for z in range(4):
            for c in range(2):
                step = (offset, 0) if c == core_axis else (0, offset)
                source = ((y + step[0]) % 4, (z + step[1]) % 4, c)
                pairs.append((source[0] * 8 + source[1] * 2 + c, y * 8 + z * 2 + c))
    return lax.ppermute(value, ("y", "z", "c"), pairs)


def along(value, offset):
    return fetch_plane(value, offset, 0)


def across(value, offset):
    return fetch_plane(value, offset, 1)


def rotated(value, start, axis):
    twice = jnp.concatenate([value, value], axis=axis)
    return lax.dynamic_slice_in_dim(twice, start, value.shape[axis], axis)


def attend_local(query_cols, keys, values, lengths):
    seq_rows, patch_len, heads_width = keys.shape
    head_count = heads_width // HEAD_DIM
    query_heads = query_cols.reshape(seq_rows, head_count, HEAD_DIM)
    key_heads = keys.reshape(seq_rows, patch_len, head_count, HEAD_DIM)
    value_heads = values.reshape(seq_rows, patch_len, head_count, HEAD_DIM)
    scores = jnp.einsum(
        "shd,sphd->shp", query_heads, key_heads, preferred_element_type=F32
    ) * HEAD_DIM ** (-0.5)
    live_mask = jnp.arange(patch_len, dtype=jnp.int32)[None, None, :] < lengths[:, None, None]
    scores = jnp.where(live_mask, scores, F32(-1e30))
    top_score = jnp.max(scores, axis=2, keepdims=True)
    expo = jnp.where(live_mask, jnp.exp(scores - top_score), F32(0.0))
    weights = (expo / jnp.sum(expo, axis=2, keepdims=True)).astype(BF16)
    mixed = jnp.einsum("shp,sphd->shd", weights, value_heads, preferred_element_type=F32)
    return mixed.astype(BF16).reshape(seq_rows, heads_width)


def norm_kernel(order_ref, state_ref, mine_ref, other_ref, gain_ref, state_out, rows_out, scratch):
    update = mine_ref[...].astype(F32) + other_ref[...].astype(F32)
    state = state_ref[...] + update.astype(BF16).astype(F32)
    state_out[...] = state
    mean_square = jnp.mean(state * state, axis=1, keepdims=True)
    scratch[...] = (state * lax.rsqrt(mean_square + NORM_FLOOR) * gain_ref[...]).astype(BF16)
    for j in range(16):
        start = pl.multiple_of(order_ref[j] * BLOCK, BLOCK)
        rows_out[j // 4, :, (j % 4) * BLOCK : (j % 4 + 1) * BLOCK] = scratch[:, pl.ds(start, BLOCK)]


def add_and_norm(order, state, mine, other, gain):
    rows, width = state.shape
    return pl.pallas_call(
        norm_kernel,
        out_shape=(
            jax.ShapeDtypeStruct((rows, width), F32),
            jax.ShapeDtypeStruct((4, rows, width // 4), BF16),
        ),
        in_specs=[pl.BlockSpec(memory_space=pltpu.SMEM)] + [pl.BlockSpec(memory_space=pltpu.VMEM)] * 4,
        out_specs=(pl.BlockSpec(memory_space=pltpu.VMEM),) * 2,
        scratch_shapes=[pltpu.VMEM((rows, width), BF16)],
        name="add_and_norm",
    )(order, state, mine, other, gain[None, :])


def place_kernel(order_ref, *refs):
    out_ref = refs[-1]
    for j in range(16):
        start = pl.multiple_of(order_ref[j] * BLOCK, BLOCK)
        out_ref[:, pl.ds(start, BLOCK)] = refs[j // 4][:, (j % 4) * BLOCK : (j % 4 + 1) * BLOCK]


def natural_columns(order, quarters):
    rows, width = quarters[0].shape
    return pl.pallas_call(
        place_kernel,
        out_shape=jax.ShapeDtypeStruct((rows, 4 * width), BF16),
        in_specs=[pl.BlockSpec(memory_space=pltpu.SMEM)] + [pl.BlockSpec(memory_space=pltpu.VMEM)] * 4,
        out_specs=pl.BlockSpec(memory_space=pltpu.VMEM),
        name="natural_columns",
    )(order, *quarters)


def gather_weight(block):
    far = across(block, 2)
    return block, across(block, 1), far, across(block, 3)


def reduce_x(pieces):
    arrived = [fetch(pieces((-step) % 4), "x", step) for step in (2, 1, 3)]
    total = pieces(0).astype(F32)
    for piece in arrived:
        total = total + piece.astype(F32)
    return total.astype(BF16)


def per_device(
    patch_query,
    key_cache,
    value_cache,
    cache_len,
    patch_end,
    ended_index,
    pool_out,
    norm_gain,
    w_in,
    w_out,
):
    seq_rows, width = patch_query.shape
    heads_width = key_cache.shape[2]
    layers, block_cols, _, hidden_local = w_in.shape
    y = lax.axis_index("y")
    z = lax.axis_index("z")
    x = lax.axis_index("x")
    c = lax.axis_index("c")
    quarter = width // 4

    near = jnp.arange(4, dtype=jnp.int32)
    step_y = jnp.where(c == 0, near[:, None], near[None, :])
    step_z = jnp.where(c == 0, near[None, :], near[:, None])
    order = (((y + step_y) % 4) * 4 + (z + step_z) % 4).reshape(16).astype(jnp.int32)

    w_in_rows = lax.optimization_barrier(w_in.reshape(layers, block_cols, 2 * hidden_local))
    ins = [gather_weight(w_in_rows[layer]) for layer in range(layers)]
    outs = [gather_weight(w_out[layer].T) for layer in range(layers)]

    slots = rotated(ended_index.reshape(4, 2, 16), x, 0)
    sequence = jnp.arange(seq_rows, dtype=jnp.int32)[None, :]
    picker = (slots.reshape(128, 1) == sequence).astype(BF16)
    last_slots = rotated(slots, c, 1).transpose(1, 0, 2).reshape(128, 1)
    last_picker = (last_slots == sequence).astype(BF16)

    mp_index = x * 2 + c
    query_cols = lax.dynamic_slice_in_dim(patch_query, mp_index * heads_width, heads_width, 1)
    attended = attend_local(query_cols, key_cache, value_cache, cache_len)
    chosen = jnp.dot(picker, attended, preferred_element_type=F32).astype(BF16)
    partial = jnp.dot(chosen, pool_out, preferred_element_type=F32).astype(BF16)
    partial = partial.reshape(4, 32, width)
    mine = reduce_x(lambda r: partial[r])
    state = jnp.dot(picker[:32], patch_query, preferred_element_type=F32)
    other = fetch(mine, "c", 1)

    for layer in range(layers):
        state, blocks = add_and_norm(order, state, mine, other, norm_gain[layer])
        arrived = [along(blocks[(-s) % 4], s) for s in (1, 2, 3)]
        blocks = jnp.stack([blocks[0]] + arrived)
        far = fetch(blocks, "x", 2)
        rows = [blocks, fetch(blocks, "x", 1), far, fetch(blocks, "x", 3)]
        rows = jnp.stack(rows, axis=1).reshape(4, 128, quarter)
        weight_in = jnp.concatenate(ins[layer])
        weight_out = jnp.concatenate(outs[layer])

        def product(step):
            return jnp.dot(rows[step], weight_in, preferred_element_type=F32)

        arrived = [along(product((-s) % 4).astype(BF16), s) for s in (2, 1, 3)]
        gate_up = product(0)
        for block in arrived:
            gate_up = gate_up + block.astype(F32)
        hidden = (jax.nn.silu(gate_up[:, :hidden_local]) * gate_up[:, hidden_local:]).astype(BF16)
        far = along(hidden, 2)
        all_hidden = jnp.concatenate([hidden, along(hidden, 1), far, along(hidden, 3)])
        partial = lax.dot_general(
            all_hidden, weight_out, (((1,), (1,)), ((), ())), preferred_element_type=F32
        ).astype(BF16)
        partial = partial.reshape(4, 4, 32, quarter)
        reduced = reduce_x(lambda r: partial[:, r])
        arrived = [along(reduced[(-s) % 4], s) for s in (1, 2, 3)]
        mine = natural_columns(order, [reduced[0]] + arrived)
        other = fetch(mine, "c", 1)

    update = mine.astype(F32) + other.astype(F32)
    state = (state + update.astype(BF16).astype(F32)).astype(BF16)
    piece = lax.dynamic_slice_in_dim(state, c * 16, 16, 0)
    far = fetch(piece, "x", 2)
    own_core = jnp.stack([piece, fetch(piece, "x", 1), far, fetch(piece, "x", 3)])
    whole = jnp.stack([own_core, fetch(own_core, "c", 1)]).reshape(128, width)
    placed = lax.dot_general(last_picker, whole, (((0,), (0,)), ((), ())), preferred_element_type=F32)
    return (placed * patch_end.astype(F32)[:, None]).astype(BF16)


def solution(mesh):
    torus = Mesh(mesh.devices.reshape(4, 4, 4, 2), ("y", "z", "x", "c"))
    dp, mp = ("y", "z"), ("x", "c")
    in_specs = (
        P(dp, None),
        P(dp, None, mp),
        P(dp, None, mp),
        P(dp),
        P(dp),
        P(dp),
        P(mp, None),
        P(),
        P(None, dp, None, mp),
        P(None, mp, dp),
    )
    return jax.shard_map(
        per_device, mesh=torus, in_specs=in_specs, out_specs=P(dp, None), check_vma=False
    )
```

```python
import jax
import jax.numpy as jnp
from jax import lax
from jax.experimental import pallas as pl
from jax.experimental.pallas import tpu as pltpu
from jax.sharding import Mesh, PartitionSpec as P


HEAD_DIM = 128
NORM_FLOOR = 1e-05
BF16 = jnp.bfloat16
F32 = jnp.float32
BLOCK = 256


def fetch(value, axis, offset):
    size = lax.axis_size(axis)
    return lax.ppermute(value, axis, [(j, (j - offset) % size) for j in range(size)])


def fetch_plane(value, offset, core_axis):
    pairs = []
    for y in range(4):
        for z in range(4):
            for c in range(2):
                step = (offset, 0) if c == core_axis else (0, offset)
                source = ((y + step[0]) % 4, (z + step[1]) % 4, c)
                pairs.append((source[0] * 8 + source[1] * 2 + c, y * 8 + z * 2 + c))
    return lax.ppermute(value, ("y", "z", "c"), pairs)


def along(value, offset):
    return fetch_plane(value, offset, 0)


def across(value, offset):
    return fetch_plane(value, offset, 1)


def rotated(value, start, axis):
    twice = jnp.concatenate([value, value], axis=axis)
    return lax.dynamic_slice_in_dim(twice, start, value.shape[axis], axis)


def attend_local(query_cols, keys, values, lengths):
    seq_rows, patch_len, heads_width = keys.shape
    head_count = heads_width // HEAD_DIM
    query_heads = query_cols.reshape(seq_rows, head_count, HEAD_DIM)
    key_heads = keys.reshape(seq_rows, patch_len, head_count, HEAD_DIM)
    value_heads = values.reshape(seq_rows, patch_len, head_count, HEAD_DIM)
    scores = jnp.einsum(
        "shd,sphd->shp", query_heads, key_heads, preferred_element_type=F32
    ) * HEAD_DIM ** (-0.5)
    live_mask = jnp.arange(patch_len, dtype=jnp.int32)[None, None, :] < lengths[:, None, None]
    scores = jnp.where(live_mask, scores, F32(-1e30))
    top_score = jnp.max(scores, axis=2, keepdims=True)
    expo = jnp.where(live_mask, jnp.exp(scores - top_score), F32(0.0))
    weights = (expo / jnp.sum(expo, axis=2, keepdims=True)).astype(BF16)
    mixed = jnp.einsum("shp,sphd->shd", weights, value_heads, preferred_element_type=F32)
    return mixed.astype(BF16).reshape(seq_rows, heads_width)


def norm_kernel(order_ref, state_ref, mine_ref, other_ref, gain_ref, state_out, rows_out, scratch):
    update = mine_ref[...].astype(F32) + other_ref[...].astype(F32)
    state = state_ref[...] + update.astype(BF16).astype(F32)
    state_out[...] = state
    mean_square = jnp.mean(state * state, axis=1, keepdims=True)
    scratch[...] = (state * lax.rsqrt(mean_square + NORM_FLOOR) * gain_ref[...]).astype(BF16)
    for j in range(16):
        start = pl.multiple_of(order_ref[j] * BLOCK, BLOCK)
        block = scratch[:, pl.ds(start, BLOCK)]
        for x in range(4):
            rows_out[j // 4, x, :, (j % 4) * BLOCK : (j % 4 + 1) * BLOCK] = block


def vmem_specs(count):
    return [pl.BlockSpec(memory_space=pltpu.VMEM)] * count


def add_and_norm(order, state, mine, other, gain):
    rows, width = state.shape
    return pl.pallas_call(
        norm_kernel,
        out_shape=(
            jax.ShapeDtypeStruct((rows, width), F32),
            jax.ShapeDtypeStruct((4, 4, rows, width // 4), BF16),
        ),
        in_specs=[pl.BlockSpec(memory_space=pltpu.SMEM)] + vmem_specs(4),
        out_specs=tuple(vmem_specs(2)),
        scratch_shapes=[pltpu.VMEM((rows, width), BF16)],
        name="add_and_norm",
    )(order, state, mine, other, gain[None, :])


def place_kernel(order_ref, parts_ref, out_ref):
    for j in range(16):
        columns = slice((j % 4) * BLOCK, (j % 4 + 1) * BLOCK)
        total = parts_ref[j // 4, 0, :, columns].astype(F32)
        for x in range(1, 4):
            total = total + parts_ref[j // 4, x, :, columns].astype(F32)
        start = pl.multiple_of(order_ref[j] * BLOCK, BLOCK)
        out_ref[:, pl.ds(start, BLOCK)] = total.astype(BF16)


def summed_columns(order, parts):
    rows, width = parts.shape[2:]
    return pl.pallas_call(
        place_kernel,
        out_shape=jax.ShapeDtypeStruct((rows, 4 * width), BF16),
        in_specs=[pl.BlockSpec(memory_space=pltpu.SMEM)] + vmem_specs(1),
        out_specs=vmem_specs(1)[0],
        name="summed_columns",
    )(order, parts)


def run_copies(sems, pairs):
    copies = [pltpu.make_async_copy(src, dst, sems.at[i]) for i, (src, dst) in enumerate(pairs)]
    for copy in copies:
        copy.start()
    for copy in copies:
        copy.wait()


def layer_rows(weights, layer, count):
    rows = weights.shape[1] // count

    def kernel(weights_ref, *refs):
        source = weights_ref.at[layer]
        run_copies(
            refs[-1], [(source.at[pl.ds(i * rows, rows)], ref) for i, ref in enumerate(refs[:-1])]
        )

    return pl.pallas_call(
        kernel,
        out_shape=(jax.ShapeDtypeStruct((rows, *weights.shape[2:]), weights.dtype),) * count,
        in_specs=[pl.BlockSpec(memory_space=pl.ANY)],
        out_specs=tuple(vmem_specs(count)),
        scratch_shapes=[pltpu.SemaphoreType.DMA((count,))],
        name="layer_rows",
    )(weights)


def weave_in(pieces, parts):
    rows, width = pieces[0].shape

    def kernel(*refs):
        pieces_refs, outs, sems = refs[: len(pieces)], refs[len(pieces) : -1], refs[-1]
        pairs = []
        for out_ref, (start, count) in zip(outs, parts):
            for i, piece in enumerate(pieces_refs):
                for side in range(2):
                    columns = pl.ds(side * (width // 2) + start, count)
                    place = out_ref.at[pl.ds(i * rows, rows), pl.ds(side * count, count)]
                    pairs.append((piece.at[:, columns], place))
        run_copies(sems, pairs)

    return pl.pallas_call(
        kernel,
        out_shape=tuple(
            jax.ShapeDtypeStruct((len(pieces) * rows, 2 * count), BF16) for _, count in parts
        ),
        in_specs=[pl.BlockSpec(memory_space=pl.ANY)] * len(pieces),
        out_specs=tuple(vmem_specs(len(parts))),
        scratch_shapes=[pltpu.SemaphoreType.DMA((2 * len(parts) * len(pieces),))],
        name="weave_in",
    )(*pieces)


def weave_out(blocks):
    rows, width = blocks[0].shape

    def kernel(*refs):
        out_ref, sems = refs[-2:]
        run_copies(
            sems, [(ref, out_ref.at[:, pl.ds(i * width, width)]) for i, ref in enumerate(refs[:-2])]
        )

    return pl.pallas_call(
        kernel,
        out_shape=jax.ShapeDtypeStruct((rows, len(blocks) * width), BF16),
        in_specs=[pl.BlockSpec(memory_space=pl.ANY)] * len(blocks),
        out_specs=vmem_specs(1)[0],
        scratch_shapes=[pltpu.SemaphoreType.DMA((len(blocks),))],
        name="weave_out",
    )(*blocks)


GROUPS = [
    [((y * 4 + z) * 4 + x) * 2 + c for y, z in members for x in range(4)]
    for c in range(2)
    for members in (
        [[(a, b) if c == 0 else (b, a) for a in range(4)] for b in range(4)]
    )
]


def exchange(blocks):
    flat = blocks.reshape(16, *blocks.shape[2:])
    flat = lax.all_to_all(
        flat, ("y", "z", "x", "c"), 0, 0, axis_index_groups=GROUPS, tiled=True
    )
    return flat.reshape(blocks.shape)


def gather_forwarding(halves):
    top, low = halves
    next_top, next_low = across(top, 1), across(low, 1)
    back_top, back_low = across(top, 3), across(low, 3)
    far_top, far_low = across(next_top, 1), across(back_low, 3)
    return top, low, next_top, next_low, far_top, far_low, back_top, back_low


def gather_weight(block):
    far = across(block, 2)
    return block, across(block, 1), far, across(block, 3)


def reduce_x(pieces):
    arrived = [fetch(pieces((-step) % 4), "x", step) for step in (2, 1, 3)]
    total = pieces(0).astype(F32)
    for piece in arrived:
        total = total + piece.astype(F32)
    return total.astype(BF16)


def per_device(
    patch_query,
    key_cache,
    value_cache,
    cache_len,
    patch_end,
    ended_index,
    pool_out,
    norm_gain,
    w_in,
    w_out,
):
    seq_rows, width = patch_query.shape
    heads_width = key_cache.shape[2]
    layers, _, _, hidden_local = w_in.shape
    y = lax.axis_index("y")
    z = lax.axis_index("z")
    x = lax.axis_index("x")
    c = lax.axis_index("c")
    quarter = width // 4

    own = jnp.where(c == 0, y, z)
    side = jnp.where(c == 0, z, y)
    position = jnp.arange(4, dtype=jnp.int32)
    first = position[:, None]
    second = (side + position[None, :]) % 4
    order = jnp.where(c == 0, first * 4 + second, second * 4 + first).reshape(16).astype(jnp.int32)
    large = hidden_local // 7 * 4
    parts = ((0, large), (large, hidden_local - large))

    def weights_of(layer, w_in, w_out):
        rows = layer_rows(w_in, layer, 2 if layer else 1)
        rows = [piece.reshape(-1, 2 * hidden_local) for piece in rows]
        gathered = gather_forwarding(rows) if layer else gather_weight(rows[0])
        return gathered, gather_weight(w_out[layer])

    ins, outs = weights_of(0, w_in, w_out)

    slots = rotated(ended_index.reshape(4, 2, 16), x, 0)
    sequence = jnp.arange(seq_rows, dtype=jnp.int32)[None, :]
    picker = (slots.reshape(128, 1) == sequence).astype(BF16)
    last_slots = rotated(slots, c, 1).transpose(1, 0, 2).reshape(128, 1)
    last_picker = (last_slots == sequence).astype(BF16)

    mp_index = x * 2 + c
    query_cols = lax.dynamic_slice_in_dim(patch_query, mp_index * heads_width, heads_width, 1)
    attended = attend_local(query_cols, key_cache, value_cache, cache_len)
    chosen = jnp.dot(picker, attended, preferred_element_type=F32).astype(BF16)
    partial = jnp.dot(chosen, pool_out, preferred_element_type=F32).astype(BF16)
    partial = partial.reshape(4, 32, width)
    mine = reduce_x(lambda r: partial[r])
    state = jnp.dot(picker[:32], patch_query, preferred_element_type=F32)
    other = fetch(mine, "c", 1)

    for layer in range(layers):
        state, blocks = add_and_norm(order, state, mine, other, norm_gain[layer])
        rows = exchange(blocks).reshape(4, 128, quarter)
        rows = rotated(rows, own, 0).reshape(512, quarter)
        halves = weave_in(ins, parts)
        products = []
        for part in range(2):
            products.append(jnp.dot(rows, halves[part], preferred_element_type=F32).astype(BF16))
        weight_out = weave_out(outs)
        if layer + 1 < layers:
            w_in, w_out, _ = lax.optimization_barrier((w_in, w_out, blocks))
            ins, outs = weights_of(layer + 1, w_in, w_out)
        partial = 0.0
        for part, (start, count) in enumerate(parts):
            product = products[part].reshape(4, 128, 2 * count)
            arrived = [along(product[(-s) % 4], s) for s in (2, 1, 3)]
            gate_up = product[0].astype(F32)
            for block in arrived:
                gate_up = gate_up + block.astype(F32)
            hidden = (jax.nn.silu(gate_up[:, :count]) * gate_up[:, count:]).astype(BF16)
            far = along(hidden, 2)
            all_hidden = jnp.concatenate([hidden, along(hidden, 1), far, along(hidden, 3)])
            partial = partial + jnp.dot(
                all_hidden, weight_out[start : start + count], preferred_element_type=F32
            )
        partial = rotated(partial.astype(BF16).reshape(4, 4, 32, quarter), (4 - own) % 4, 0)
        partial = exchange(partial)
        mine = summed_columns(order, partial)
        other = fetch(mine, "c", 1)

    update = mine.astype(F32) + other.astype(F32)
    state = (state + update.astype(BF16).astype(F32)).astype(BF16)
    piece = lax.dynamic_slice_in_dim(state, c * 16, 16, 0)
    far = fetch(piece, "x", 2)
    own_core = jnp.stack([piece, fetch(piece, "x", 1), far, fetch(piece, "x", 3)])
    whole = jnp.stack([own_core, fetch(own_core, "c", 1)]).reshape(128, width)
    placed = lax.dot_general(last_picker, whole, (((0,), (0,)), ((), ())), preferred_element_type=F32)
    return (placed * patch_end.astype(F32)[:, None]).astype(BF16)


def solution(mesh):
    torus = Mesh(mesh.devices.reshape(4, 4, 4, 2), ("y", "z", "x", "c"))
    dp, mp = ("y", "z"), ("x", "c")
    in_specs = (
        P(dp, None),
        P(dp, None, mp),
        P(dp, None, mp),
        P(dp),
        P(dp),
        P(dp),
        P(mp, None),
        P(),
        P(None, dp, None, mp),
        P(None, mp, dp),
    )
    return jax.shard_map(
        per_device, mesh=torus, in_specs=in_specs, out_specs=P(dp, None), check_vma=False
    )
```

```python
import jax
import jax.numpy as jnp
from jax import lax
from jax.experimental import pallas as pl
from jax.experimental.pallas import tpu as pltpu
from jax.sharding import Mesh, PartitionSpec as P


HEAD_DIM = 128
NORM_FLOOR = 1e-05
BF16 = jnp.bfloat16
F32 = jnp.float32
BLOCK = 256
KERNEL_VMEM = 6 * 2**20
WOVEN_VMEM = 10 * 2**20


def fetch(value, axis, offset):
    size = lax.axis_size(axis)
    return lax.ppermute(value, axis, [(j, (j - offset) % size) for j in range(size)])


def fetch_plane(value, offset, core_axis):
    pairs = []
    for y in range(4):
        for z in range(4):
            for c in range(2):
                step = (offset, 0) if c == core_axis else (0, offset)
                source = ((y + step[0]) % 4, (z + step[1]) % 4, c)
                pairs.append((source[0] * 8 + source[1] * 2 + c, y * 8 + z * 2 + c))
    return lax.ppermute(value, ("y", "z", "c"), pairs)


def along(value, offset):
    return fetch_plane(value, offset, 0)


def across(value, offset):
    return fetch_plane(value, offset, 1)


def rotated(value, start, axis):
    twice = jnp.concatenate([value, value], axis=axis)
    return lax.dynamic_slice_in_dim(twice, start, value.shape[axis], axis)


def attend_local(query_cols, keys, values, lengths):
    seq_rows, patch_len, heads_width = keys.shape
    head_count = heads_width // HEAD_DIM
    query_heads = query_cols.reshape(seq_rows, head_count, HEAD_DIM)
    key_heads = keys.reshape(seq_rows, patch_len, head_count, HEAD_DIM)
    value_heads = values.reshape(seq_rows, patch_len, head_count, HEAD_DIM)
    scores = jnp.einsum(
        "shd,sphd->shp", query_heads, key_heads, preferred_element_type=F32
    ) * HEAD_DIM ** (-0.5)
    live_mask = jnp.arange(patch_len, dtype=jnp.int32)[None, None, :] < lengths[:, None, None]
    scores = jnp.where(live_mask, scores, F32(-1e30))
    top_score = jnp.max(scores, axis=2, keepdims=True)
    expo = jnp.where(live_mask, jnp.exp(scores - top_score), F32(0.0))
    weights = (expo / jnp.sum(expo, axis=2, keepdims=True)).astype(BF16)
    mixed = jnp.einsum("shp,sphd->shd", weights, value_heads, preferred_element_type=F32)
    return mixed.astype(BF16).reshape(seq_rows, heads_width)


def norm_kernel(order_ref, state_ref, mine_ref, other_ref, gain_ref, state_out, rows_out, scratch):
    update = mine_ref[...].astype(F32) + other_ref[...].astype(F32)
    state = state_ref[...] + update.astype(BF16).astype(F32)
    state_out[...] = state
    mean_square = jnp.mean(state * state, axis=1, keepdims=True)
    scratch[...] = (state * lax.rsqrt(mean_square + NORM_FLOOR) * gain_ref[...]).astype(BF16)
    for j in range(16):
        start = pl.multiple_of(order_ref[j] * BLOCK, BLOCK)
        block = scratch[:, pl.ds(start, BLOCK)]
        for x in range(4):
            rows_out[j // 4, x, :, (j % 4) * BLOCK : (j % 4 + 1) * BLOCK] = block


def vmem_specs(count):
    return [pl.BlockSpec(memory_space=pltpu.VMEM)] * count


def add_and_norm(order, state, mine, other, gain):
    rows, width = state.shape
    return pl.pallas_call(
        norm_kernel,
        out_shape=(
            jax.ShapeDtypeStruct((rows, width), F32),
            jax.ShapeDtypeStruct((4, 4, rows, width // 4), BF16),
        ),
        in_specs=[pl.BlockSpec(memory_space=pltpu.SMEM)] + vmem_specs(4),
        out_specs=tuple(vmem_specs(2)),
        scratch_shapes=[pltpu.VMEM((rows, width), BF16)],
        compiler_params=pltpu.CompilerParams(vmem_limit_bytes=KERNEL_VMEM),
        name="add_and_norm",
    )(order, state, mine, other, gain[None, :])


def place_kernel(order_ref, parts_ref, out_ref):
    for j in range(16):
        columns = slice((j % 4) * BLOCK, (j % 4 + 1) * BLOCK)
        total = parts_ref[j // 4, 0, :, columns].astype(F32)
        for x in range(1, 4):
            total = total + parts_ref[j // 4, x, :, columns].astype(F32)
        start = pl.multiple_of(order_ref[j] * BLOCK, BLOCK)
        out_ref[:, pl.ds(start, BLOCK)] = total.astype(BF16)


def summed_columns(order, parts):
    rows, width = parts.shape[2:]
    return pl.pallas_call(
        place_kernel,
        out_shape=jax.ShapeDtypeStruct((rows, 4 * width), BF16),
        in_specs=[pl.BlockSpec(memory_space=pltpu.SMEM)] + vmem_specs(1),
        out_specs=vmem_specs(1)[0],
        compiler_params=pltpu.CompilerParams(vmem_limit_bytes=KERNEL_VMEM),
        name="summed_columns",
    )(order, parts)


def run_copies(sems, pairs):
    copies = [pltpu.make_async_copy(src, dst, sems.at[i]) for i, (src, dst) in enumerate(pairs)]
    for copy in copies:
        copy.start()
    for copy in copies:
        copy.wait()


def layer_rows(weights, layer, count):
    rows = weights.shape[1] // count

    def kernel(weights_ref, *refs):
        source = weights_ref.at[layer]
        run_copies(
            refs[-1], [(source.at[pl.ds(i * rows, rows)], ref) for i, ref in enumerate(refs[:-1])]
        )

    return pl.pallas_call(
        kernel,
        out_shape=(pltpu.VMEM((rows, *weights.shape[2:]), weights.dtype),) * count,
        in_specs=[pl.BlockSpec(memory_space=pltpu.HBM)],
        out_specs=tuple(vmem_specs(count)),
        scratch_shapes=[pltpu.SemaphoreType.DMA((count,))],
        compiler_params=pltpu.CompilerParams(vmem_limit_bytes=KERNEL_VMEM),
        name="layer_rows",
    )(weights)


def weave_in(pieces, parts):
    rows, width = pieces[0].shape

    def kernel(*refs):
        pieces_refs, outs, sems = refs[: len(pieces)], refs[len(pieces) : -1], refs[-1]
        pairs = []
        for out_ref, (start, count) in zip(outs, parts):
            for i, piece in enumerate(pieces_refs):
                for side in range(2):
                    columns = pl.ds(side * (width // 2) + start, count)
                    place = out_ref.at[pl.ds(i * rows, rows), pl.ds(side * count, count)]
                    pairs.append((piece.at[:, columns], place))
        run_copies(sems, pairs)

    return pl.pallas_call(
        kernel,
        out_shape=tuple(
            pltpu.VMEM((len(pieces) * rows, 2 * count), BF16) for _, count in parts
        ),
        in_specs=[pl.BlockSpec(memory_space=pltpu.HBM)] * len(pieces),
        out_specs=tuple(vmem_specs(len(parts))),
        scratch_shapes=[pltpu.SemaphoreType.DMA((2 * len(parts) * len(pieces),))],
        compiler_params=pltpu.CompilerParams(vmem_limit_bytes=WOVEN_VMEM),
        name="weave_in",
    )(*pieces)


def weave_out(blocks):
    rows, width = blocks[0].shape

    def kernel(*refs):
        out_ref, sems = refs[-2:]
        run_copies(
            sems, [(ref, out_ref.at[:, pl.ds(i * width, width)]) for i, ref in enumerate(refs[:-2])]
        )

    return pl.pallas_call(
        kernel,
        out_shape=pltpu.VMEM((rows, len(blocks) * width), BF16),
        in_specs=[pl.BlockSpec(memory_space=pltpu.HBM)] * len(blocks),
        out_specs=vmem_specs(1)[0],
        scratch_shapes=[pltpu.SemaphoreType.DMA((len(blocks),))],
        compiler_params=pltpu.CompilerParams(vmem_limit_bytes=WOVEN_VMEM),
        name="weave_out",
    )(*blocks)


GROUPS = [
    [((y * 4 + z) * 4 + x) * 2 + c for y, z in members for x in range(4)]
    for c in range(2)
    for members in (
        [[(a, b) if c == 0 else (b, a) for a in range(4)] for b in range(4)]
    )
]


def exchange(blocks):
    flat = blocks.reshape(16, *blocks.shape[2:])
    flat = lax.all_to_all(
        flat, ("y", "z", "x", "c"), 0, 0, axis_index_groups=GROUPS, tiled=True
    )
    return flat.reshape(blocks.shape)


def gather_forwarding(halves):
    top, low = halves
    next_top, next_low = across(top, 1), across(low, 1)
    back_top, back_low = across(top, 3), across(low, 3)
    far_top, far_low = across(next_top, 1), across(back_low, 3)
    return top, low, next_top, next_low, far_top, far_low, back_top, back_low


def gather_weight(block):
    far = across(block, 2)
    return block, across(block, 1), far, across(block, 3)


def reduce_x(pieces):
    arrived = [fetch(pieces((-step) % 4), "x", step) for step in (2, 1, 3)]
    total = pieces(0).astype(F32)
    for piece in arrived:
        total = total + piece.astype(F32)
    return total.astype(BF16)


def per_device(
    patch_query,
    key_cache,
    value_cache,
    cache_len,
    patch_end,
    ended_index,
    pool_out,
    norm_gain,
    w_in,
    w_out,
):
    seq_rows, width = patch_query.shape
    heads_width = key_cache.shape[2]
    layers, _, _, hidden_local = w_in.shape
    y = lax.axis_index("y")
    z = lax.axis_index("z")
    x = lax.axis_index("x")
    c = lax.axis_index("c")
    quarter = width // 4

    own = jnp.where(c == 0, y, z)
    side = jnp.where(c == 0, z, y)
    position = jnp.arange(4, dtype=jnp.int32)
    first = position[:, None]
    second = (side + position[None, :]) % 4
    order = jnp.where(c == 0, first * 4 + second, second * 4 + first).reshape(16).astype(jnp.int32)
    large = hidden_local // 7 * 4
    parts = ((0, large), (large, hidden_local - large))

    def owned(product, step):
        return lax.dynamic_index_in_dim(product, (own + step) % 4, 0, keepdims=False)

    def weights_of(layer, w_in, w_out):
        rows = layer_rows(w_in, layer, 2 if layer else 1)
        rows = [piece.reshape(-1, 2 * hidden_local) for piece in rows]
        gathered = gather_forwarding(rows) if layer else gather_weight(rows[0])
        return gathered, gather_weight(w_out[layer])

    ins, outs = weights_of(0, w_in, w_out)

    slots = rotated(ended_index.reshape(4, 2, 16), x, 0)
    sequence = jnp.arange(seq_rows, dtype=jnp.int32)[None, :]
    own_picker = (slots[0].reshape(32, 1) == sequence).astype(BF16)
    picker = (rotated(slots, c, 1).reshape(128, 1) == sequence).astype(BF16)
    last_slots = rotated(slots, c, 1).transpose(1, 0, 2).reshape(128, 1)
    last_picker = (last_slots == sequence).astype(BF16)

    mp_index = x * 2 + c
    query_cols = lax.dynamic_slice_in_dim(patch_query, mp_index * heads_width, heads_width, 1)
    attended = attend_local(query_cols, key_cache, value_cache, cache_len)
    chosen = jnp.dot(picker, attended, preferred_element_type=F32).astype(BF16)
    partial = jnp.dot(chosen, pool_out, preferred_element_type=F32).astype(BF16)
    partial = partial.reshape(4, 2, 16, width)
    other = fetch(partial[:, 1], "c", 1)
    partial = (partial[:, 0].astype(F32) + other.astype(F32)).astype(BF16)
    mine = reduce_x(lambda r: partial[r])
    other = fetch(mine, "c", 1)
    first, second = jnp.where(c == 0, mine, other), jnp.where(c == 0, other, mine)
    mine = jnp.concatenate([first, second])
    other = jnp.zeros_like(mine)
    state = jnp.dot(own_picker, patch_query, preferred_element_type=F32)

    for layer in range(layers):
        state, blocks = add_and_norm(order, state, mine, other, norm_gain[layer])
        rows = exchange(blocks).reshape(4, 128, quarter)
        rows = rows.reshape(512, quarter)
        halves = weave_in(ins, parts)
        products = []
        for part in range(2):
            products.append(jnp.dot(rows, halves[part], preferred_element_type=F32).astype(BF16))
        weight_out = weave_out(outs)
        if layer + 1 < layers:
            w_in, w_out, _ = lax.optimization_barrier((w_in, w_out, blocks))
            ins, outs = weights_of(layer + 1, w_in, w_out)
        partial = 0.0
        for part, (start, count) in enumerate(parts):
            product = products[part].reshape(4, 128, 2 * count)
            arrived = [along(owned(product, -s), s) for s in (2, 1, 3)]
            gate_up = owned(product, 0).astype(F32)
            for block in arrived:
                gate_up = gate_up + block.astype(F32)
            hidden = (jax.nn.silu(gate_up[:, :count]) * gate_up[:, count:]).astype(BF16)
            far = along(hidden, 2)
            all_hidden = jnp.concatenate([hidden, along(hidden, 1), far, along(hidden, 3)])
            partial = partial + jnp.dot(
                all_hidden, weight_out[start : start + count], preferred_element_type=F32
            )
        partial = rotated(partial.astype(BF16).reshape(4, 4, 32, quarter), (4 - own) % 4, 0)
        partial = exchange(partial)
        mine = summed_columns(order, partial)
        other = fetch(mine, "c", 1)

    update = mine.astype(F32) + other.astype(F32)
    state = (state + update.astype(BF16).astype(F32)).astype(BF16)
    piece = lax.dynamic_slice_in_dim(state, c * 16, 16, 0)
    far = fetch(piece, "x", 2)
    own_core = jnp.stack([piece, fetch(piece, "x", 1), far, fetch(piece, "x", 3)])
    whole = jnp.stack([own_core, fetch(own_core, "c", 1)]).reshape(128, width)
    placed = lax.dot_general(last_picker, whole, (((0,), (0,)), ((), ())), preferred_element_type=F32)
    return (placed * patch_end.astype(F32)[:, None]).astype(BF16)


def solution(mesh):
    torus = Mesh(mesh.devices.reshape(4, 4, 4, 2), ("y", "z", "x", "c"))
    dp, mp = ("y", "z"), ("x", "c")
    in_specs = (
        P(dp, None),
        P(dp, None, mp),
        P(dp, None, mp),
        P(dp),
        P(dp),
        P(dp),
        P(mp, None),
        P(),
        P(None, dp, None, mp),
        P(None, mp, dp),
    )
    return jax.shard_map(
        per_device, mesh=torus, in_specs=in_specs, out_specs=P(dp, None), check_vma=False
    )
```

```python
import jax
import jax.numpy as jnp
from jax import lax
from jax.experimental import pallas as pl
from jax.experimental.pallas import tpu as pltpu
from jax.sharding import Mesh, PartitionSpec as P


HEAD_DIM = 128
NORM_FLOOR = 1e-05
BF16 = jnp.bfloat16
F32 = jnp.float32
BLOCK = 256
KERNEL_VMEM = 6 * 2**20
WOVEN_VMEM = 10 * 2**20


def fetch(value, axis, offset):
    size = lax.axis_size(axis)
    return lax.ppermute(value, axis, [(j, (j - offset) % size) for j in range(size)])


def fetch_plane(value, offset, core_axis):
    pairs = []
    for y in range(4):
        for z in range(4):
            for c in range(2):
                step = (offset, 0) if c == core_axis else (0, offset)
                source = ((y + step[0]) % 4, (z + step[1]) % 4, c)
                pairs.append((source[0] * 8 + source[1] * 2 + c, y * 8 + z * 2 + c))
    return lax.ppermute(value, ("y", "z", "c"), pairs)


def along(value, offset):
    return fetch_plane(value, offset, 0)


def across(value, offset):
    return fetch_plane(value, offset, 1)


def rotated(value, start, axis):
    twice = jnp.concatenate([value, value], axis=axis)
    return lax.dynamic_slice_in_dim(twice, start, value.shape[axis], axis)


def attend_local(query_cols, keys, values, lengths):
    seq_rows, patch_len, heads_width = keys.shape
    head_count = heads_width // HEAD_DIM
    query_heads = query_cols.reshape(seq_rows, head_count, HEAD_DIM)
    key_heads = keys.reshape(seq_rows, patch_len, head_count, HEAD_DIM)
    value_heads = values.reshape(seq_rows, patch_len, head_count, HEAD_DIM)
    scores = jnp.einsum(
        "shd,sphd->shp", query_heads, key_heads, preferred_element_type=F32
    ) * HEAD_DIM ** (-0.5)
    live_mask = jnp.arange(patch_len, dtype=jnp.int32)[None, None, :] < lengths[:, None, None]
    scores = jnp.where(live_mask, scores, F32(-1e30))
    top_score = jnp.max(scores, axis=2, keepdims=True)
    expo = jnp.where(live_mask, jnp.exp(scores - top_score), F32(0.0))
    weights = (expo / jnp.sum(expo, axis=2, keepdims=True)).astype(BF16)
    mixed = jnp.einsum("shp,sphd->shd", weights, value_heads, preferred_element_type=F32)
    return mixed.astype(BF16).reshape(seq_rows, heads_width)


def norm_kernel(order_ref, state_ref, mine_ref, other_ref, gain_ref, state_out, rows_out, scratch):
    update = mine_ref[...].astype(F32) + other_ref[...].astype(F32)
    state = state_ref[...] + update.astype(BF16).astype(F32)
    state_out[...] = state
    mean_square = jnp.mean(state * state, axis=1, keepdims=True)
    scratch[...] = (state * lax.rsqrt(mean_square + NORM_FLOOR) * gain_ref[...]).astype(BF16)
    for j in range(16):
        start = pl.multiple_of(order_ref[j] * BLOCK, BLOCK)
        block = scratch[:, pl.ds(start, BLOCK)]
        for x in range(4):
            rows_out[j // 4, x, :, (j % 4) * BLOCK : (j % 4 + 1) * BLOCK] = block


def vmem_specs(count):
    return [pl.BlockSpec(memory_space=pltpu.VMEM)] * count


def add_and_norm(order, state, mine, other, gain):
    rows, width = state.shape
    return pl.pallas_call(
        norm_kernel,
        out_shape=(
            jax.ShapeDtypeStruct((rows, width), F32),
            jax.ShapeDtypeStruct((4, 4, rows, width // 4), BF16),
        ),
        in_specs=[pl.BlockSpec(memory_space=pltpu.SMEM)] + vmem_specs(4),
        out_specs=tuple(vmem_specs(2)),
        scratch_shapes=[pltpu.VMEM((rows, width), BF16)],
        compiler_params=pltpu.CompilerParams(vmem_limit_bytes=KERNEL_VMEM),
        name="add_and_norm",
    )(order, state, mine, other, gain[None, :])


def place_kernel(order_ref, parts_ref, out_ref):
    for j in range(16):
        columns = slice((j % 4) * BLOCK, (j % 4 + 1) * BLOCK)
        total = parts_ref[j // 4, 0, :, columns].astype(F32)
        for x in range(1, 4):
            total = total + parts_ref[j // 4, x, :, columns].astype(F32)
        start = pl.multiple_of(order_ref[j] * BLOCK, BLOCK)
        out_ref[:, pl.ds(start, BLOCK)] = total.astype(BF16)


def summed_columns(order, parts):
    rows, width = parts.shape[2:]
    return pl.pallas_call(
        place_kernel,
        out_shape=jax.ShapeDtypeStruct((rows, 4 * width), BF16),
        in_specs=[pl.BlockSpec(memory_space=pltpu.SMEM)] + vmem_specs(1),
        out_specs=vmem_specs(1)[0],
        compiler_params=pltpu.CompilerParams(vmem_limit_bytes=KERNEL_VMEM),
        name="summed_columns",
    )(order, parts)


def run_copies(sems, pairs):
    copies = [pltpu.make_async_copy(src, dst, sems.at[i]) for i, (src, dst) in enumerate(pairs)]
    for copy in copies:
        copy.start()
    for copy in copies:
        copy.wait()


def layer_rows(weights, layer, count):
    rows = weights.shape[1] // count

    def kernel(weights_ref, *refs):
        source = weights_ref.at[layer]
        run_copies(
            refs[-1], [(source.at[pl.ds(i * rows, rows)], ref) for i, ref in enumerate(refs[:-1])]
        )

    return pl.pallas_call(
        kernel,
        out_shape=(pltpu.VMEM((rows, *weights.shape[2:]), weights.dtype),) * count,
        in_specs=[pl.BlockSpec(memory_space=pltpu.HBM)],
        out_specs=tuple(vmem_specs(count)),
        scratch_shapes=[pltpu.SemaphoreType.DMA((count,))],
        compiler_params=pltpu.CompilerParams(vmem_limit_bytes=KERNEL_VMEM),
        name="layer_rows",
    )(weights)


def weave_in(pieces, parts):
    rows, width = pieces[0].shape

    def kernel(*refs):
        pieces_refs, outs, sems = refs[: len(pieces)], refs[len(pieces) : -1], refs[-1]
        pairs = []
        for out_ref, (start, count) in zip(outs, parts):
            for i, piece in enumerate(pieces_refs):
                for side in range(2):
                    columns = pl.ds(side * (width // 2) + start, count)
                    place = out_ref.at[pl.ds(i * rows, rows), pl.ds(side * count, count)]
                    pairs.append((piece.at[:, columns], place))
        run_copies(sems, pairs)

    return pl.pallas_call(
        kernel,
        out_shape=tuple(
            jax.ShapeDtypeStruct((len(pieces) * rows, 2 * count), BF16) for _, count in parts
        ),
        in_specs=[pl.BlockSpec(memory_space=pltpu.HBM)] * len(pieces),
        out_specs=(pl.BlockSpec(memory_space=pltpu.HBM),) * len(parts),
        scratch_shapes=[pltpu.SemaphoreType.DMA((2 * len(parts) * len(pieces),))],
        compiler_params=pltpu.CompilerParams(vmem_limit_bytes=WOVEN_VMEM),
        name="weave_in",
    )(*pieces)


def weave_out(pieces):
    rows, width = pieces[0].shape
    low = rows // 2
    places = [(0, 0), (0, 1), (0, 2), (low, 2), (0, 3)]

    def kernel(*refs):
        out_ref, sems = refs[-2:]
        pairs = []
        for ref, piece, (row, column) in zip(refs, pieces, places):
            columns = pl.ds(column * width, width)
            pairs.append((ref, out_ref.at[pl.ds(row, piece.shape[0]), columns]))
        run_copies(sems, pairs)

    return pl.pallas_call(
        kernel,
        out_shape=pltpu.VMEM((rows, 4 * width), BF16),
        in_specs=[pl.BlockSpec(memory_space=pltpu.HBM)] * len(pieces),
        out_specs=vmem_specs(1)[0],
        scratch_shapes=[pltpu.SemaphoreType.DMA((len(pieces),))],
        compiler_params=pltpu.CompilerParams(vmem_limit_bytes=WOVEN_VMEM),
        name="weave_out",
    )(*pieces)


GROUPS = [
    [((y * 4 + z) * 4 + x) * 2 + c for y, z in members for x in range(4)]
    for c in range(2)
    for members in (
        [[(a, b) if c == 0 else (b, a) for a in range(4)] for b in range(4)]
    )
]


def exchange(blocks):
    flat = blocks.reshape(16, *blocks.shape[2:])
    flat = lax.all_to_all(
        flat, ("y", "z", "x", "c"), 0, 0, axis_index_groups=GROUPS, tiled=True
    )
    return flat.reshape(blocks.shape)


def gather_near(block):
    return block, across(block, 1), across(block, 3)


def relay_far(near):
    block, nearest, behind = near
    half = block.shape[0] // 2
    far_top, far_low = across(nearest[:half], 1), across(behind[half:], 3)
    return block, nearest, far_top, far_low, behind


def gather_forwarding(halves):
    top, low = halves
    next_top, next_low = across(top, 1), across(low, 1)
    back_top, back_low = across(top, 3), across(low, 3)
    far_top, far_low = across(next_top, 1), across(back_low, 3)
    return top, low, next_top, next_low, far_top, far_low, back_top, back_low


def gather_weight(block):
    far = across(block, 2)
    return block, across(block, 1), far, across(block, 3)


def reduce_x(pieces):
    arrived = [fetch(pieces((-step) % 4), "x", step) for step in (2, 1, 3)]
    total = pieces(0).astype(F32)
    for piece in arrived:
        total = total + piece.astype(F32)
    return total.astype(BF16)


def per_device(
    patch_query,
    key_cache,
    value_cache,
    cache_len,
    patch_end,
    ended_index,
    pool_out,
    norm_gain,
    w_in,
    w_out,
):
    seq_rows, width = patch_query.shape
    heads_width = key_cache.shape[2]
    layers, _, _, hidden_local = w_in.shape
    y = lax.axis_index("y")
    z = lax.axis_index("z")
    x = lax.axis_index("x")
    c = lax.axis_index("c")
    quarter = width // 4

    own = jnp.where(c == 0, y, z)
    side = jnp.where(c == 0, z, y)
    position = jnp.arange(4, dtype=jnp.int32)
    first = position[:, None]
    second = (side + position[None, :]) % 4
    order = jnp.where(c == 0, first * 4 + second, second * 4 + first).reshape(16).astype(jnp.int32)
    large = hidden_local // 7 * 4
    parts = ((0, large), (large, hidden_local - large))

    def owned(product, step):
        return lax.dynamic_index_in_dim(product, (own + step) % 4, 0, keepdims=False)

    def weights_of(layer, w_in, w_out):
        rows = layer_rows(w_in, layer, 2 if layer else 1)
        rows = [piece.reshape(-1, 2 * hidden_local) for piece in rows]
        gathered = gather_forwarding(rows) if layer else gather_weight(rows[0])
        return gathered, gather_near(w_out[layer])

    ins, outs = weights_of(0, w_in, w_out)

    slots = rotated(ended_index.reshape(4, 2, 16), x, 0)
    sequence = jnp.arange(seq_rows, dtype=jnp.int32)[None, :]
    own_picker = (slots[0].reshape(32, 1) == sequence).astype(BF16)
    picker = (rotated(slots, c, 1).reshape(128, 1) == sequence).astype(BF16)
    last_slots = rotated(slots, c, 1).transpose(1, 0, 2).reshape(128, 1)
    last_picker = (last_slots == sequence).astype(BF16)

    mp_index = x * 2 + c
    query_cols = lax.dynamic_slice_in_dim(patch_query, mp_index * heads_width, heads_width, 1)
    attended = attend_local(query_cols, key_cache, value_cache, cache_len)
    chosen = jnp.dot(picker, attended, preferred_element_type=F32).astype(BF16)
    partial = jnp.dot(chosen, pool_out, preferred_element_type=F32).astype(BF16)
    partial = partial.reshape(4, 2, 16, width)
    other = fetch(partial[:, 1], "c", 1)
    partial = (partial[:, 0].astype(F32) + other.astype(F32)).astype(BF16)
    mine = reduce_x(lambda r: partial[r])
    other = fetch(mine, "c", 1)
    first, second = jnp.where(c == 0, mine, other), jnp.where(c == 0, other, mine)
    mine = jnp.concatenate([first, second])
    other = jnp.zeros_like(mine)
    state = jnp.dot(own_picker, patch_query, preferred_element_type=F32)

    for layer in range(layers):
        state, blocks = add_and_norm(order, state, mine, other, norm_gain[layer])
        rows = exchange(blocks).reshape(4, 128, quarter)
        rows = rows.reshape(512, quarter)
        rows, ins = lax.optimization_barrier((rows, ins))
        halves = weave_in(ins, parts)
        products = []
        for part in range(2):
            products.append(jnp.dot(rows, halves[part], preferred_element_type=F32).astype(BF16))
        near, _ = lax.optimization_barrier((outs, products[1]))
        weight_out = weave_out(relay_far(near))
        if layer + 1 < layers:
            w_in, w_out, _ = lax.optimization_barrier((w_in, w_out, blocks))
            ins, outs = weights_of(layer + 1, w_in, w_out)
        partial = 0.0
        for part, (start, count) in enumerate(parts):
            product = products[part].reshape(4, 128, 2 * count)
            arrived = [along(owned(product, -s), s) for s in (2, 1, 3)]
            gate_up = owned(product, 0).astype(F32)
            for block in arrived:
                gate_up = gate_up + block.astype(F32)
            hidden = (jax.nn.silu(gate_up[:, :count]) * gate_up[:, count:]).astype(BF16)
            far = along(hidden, 2)
            all_hidden = jnp.concatenate([hidden, along(hidden, 1), far, along(hidden, 3)])
            partial = partial + jnp.dot(
                all_hidden, weight_out[start : start + count], preferred_element_type=F32
            )
        partial = rotated(partial.astype(BF16).reshape(4, 4, 32, quarter), (4 - own) % 4, 0)
        partial = exchange(partial)
        mine = summed_columns(order, partial)
        other = fetch(mine, "c", 1)

    update = mine.astype(F32) + other.astype(F32)
    state = (state + update.astype(BF16).astype(F32)).astype(BF16)
    piece = lax.dynamic_slice_in_dim(state, c * 16, 16, 0)
    far = fetch(piece, "x", 2)
    own_core = jnp.stack([piece, fetch(piece, "x", 1), far, fetch(piece, "x", 3)])
    whole = jnp.stack([own_core, fetch(own_core, "c", 1)]).reshape(128, width)
    placed = lax.dot_general(last_picker, whole, (((0,), (0,)), ((), ())), preferred_element_type=F32)
    return (placed * patch_end.astype(F32)[:, None]).astype(BF16)


def solution(mesh):
    torus = Mesh(mesh.devices.reshape(4, 4, 4, 2), ("y", "z", "x", "c"))
    dp, mp = ("y", "z"), ("x", "c")
    in_specs = (
        P(dp, None),
        P(dp, None, mp),
        P(dp, None, mp),
        P(dp),
        P(dp),
        P(dp),
        P(mp, None),
        P(),
        P(None, dp, None, mp),
        P(None, mp, dp),
    )
    return jax.shard_map(
        per_device, mesh=torus, in_specs=in_specs, out_specs=P(dp, None), check_vma=False
    )
```

```python
import jax
import jax.numpy as jnp
from jax import lax
from jax.experimental import pallas as pl
from jax.experimental.pallas import tpu as pltpu
from jax.sharding import Mesh, PartitionSpec as P


HEAD_DIM = 128
NORM_FLOOR = 1e-05
BF16 = jnp.bfloat16
F32 = jnp.float32
BLOCK = 256
KERNEL_VMEM = 6 * 2**20
WOVEN_VMEM = 10 * 2**20


def fetch(value, axis, offset):
    size = lax.axis_size(axis)
    return lax.ppermute(value, axis, [(j, (j - offset) % size) for j in range(size)])


def fetch_plane(value, offset, core_axis):
    pairs = []
    for y in range(4):
        for z in range(4):
            for c in range(2):
                step = (offset, 0) if c == core_axis else (0, offset)
                source = ((y + step[0]) % 4, (z + step[1]) % 4, c)
                pairs.append((source[0] * 8 + source[1] * 2 + c, y * 8 + z * 2 + c))
    return lax.ppermute(value, ("y", "z", "c"), pairs)


def along(value, offset):
    return fetch_plane(value, offset, 0)


def across(value, offset):
    return fetch_plane(value, offset, 1)


def rotated(value, start, axis):
    twice = jnp.concatenate([value, value], axis=axis)
    return lax.dynamic_slice_in_dim(twice, start, value.shape[axis], axis)


def attend_local(query_cols, keys, values, lengths):
    seq_rows, patch_len, heads_width = keys.shape
    head_count = heads_width // HEAD_DIM
    query_heads = query_cols.reshape(seq_rows, head_count, HEAD_DIM)
    key_heads = keys.reshape(seq_rows, patch_len, head_count, HEAD_DIM)
    value_heads = values.reshape(seq_rows, patch_len, head_count, HEAD_DIM)
    scores = jnp.einsum(
        "shd,sphd->shp", query_heads, key_heads, preferred_element_type=F32
    ) * HEAD_DIM ** (-0.5)
    live_mask = jnp.arange(patch_len, dtype=jnp.int32)[None, None, :] < lengths[:, None, None]
    scores = jnp.where(live_mask, scores, F32(-1e30))
    top_score = jnp.max(scores, axis=2, keepdims=True)
    expo = jnp.where(live_mask, jnp.exp(scores - top_score), F32(0.0))
    weights = (expo / jnp.sum(expo, axis=2, keepdims=True)).astype(BF16)
    mixed = jnp.einsum("shp,sphd->shd", weights, value_heads, preferred_element_type=F32)
    return mixed.astype(BF16).reshape(seq_rows, heads_width)


def norm_kernel(order_ref, state_ref, mine_ref, other_ref, gain_ref, state_out, rows_out, scratch):
    update = mine_ref[...].astype(F32) + other_ref[...].astype(F32)
    state = state_ref[...] + update.astype(BF16).astype(F32)
    state_out[...] = state
    mean_square = jnp.mean(state * state, axis=1, keepdims=True)
    scratch[...] = (state * lax.rsqrt(mean_square + NORM_FLOOR) * gain_ref[...]).astype(BF16)
    for j in range(16):
        start = pl.multiple_of(order_ref[j] * BLOCK, BLOCK)
        block = scratch[:, pl.ds(start, BLOCK)]
        for x in range(4):
            rows_out[j // 4, x, :, (j % 4) * BLOCK : (j % 4 + 1) * BLOCK] = block


def vmem_specs(count):
    return [pl.BlockSpec(memory_space=pltpu.VMEM)] * count


def add_and_norm(order, state, mine, other, gain):
    rows, width = state.shape
    return pl.pallas_call(
        norm_kernel,
        out_shape=(
            jax.ShapeDtypeStruct((rows, width), F32),
            jax.ShapeDtypeStruct((4, 4, rows, width // 4), BF16),
        ),
        in_specs=[pl.BlockSpec(memory_space=pltpu.SMEM)] + vmem_specs(4),
        out_specs=tuple(vmem_specs(2)),
        scratch_shapes=[pltpu.VMEM((rows, width), BF16)],
        compiler_params=pltpu.CompilerParams(vmem_limit_bytes=KERNEL_VMEM),
        name="add_and_norm",
    )(order, state, mine, other, gain[None, :])


def place_kernel(order_ref, parts_ref, out_ref):
    for j in range(16):
        columns = slice((j % 4) * BLOCK, (j % 4 + 1) * BLOCK)
        total = parts_ref[j // 4, 0, :, columns].astype(F32)
        for x in range(1, 4):
            total = total + parts_ref[j // 4, x, :, columns].astype(F32)
        start = pl.multiple_of(order_ref[j] * BLOCK, BLOCK)
        out_ref[:, pl.ds(start, BLOCK)] = total.astype(BF16)


def summed_columns(order, parts):
    rows, width = parts.shape[2:]
    return pl.pallas_call(
        place_kernel,
        out_shape=jax.ShapeDtypeStruct((rows, 4 * width), BF16),
        in_specs=[pl.BlockSpec(memory_space=pltpu.SMEM)] + vmem_specs(1),
        out_specs=vmem_specs(1)[0],
        compiler_params=pltpu.CompilerParams(vmem_limit_bytes=KERNEL_VMEM),
        name="summed_columns",
    )(order, parts)


def run_copies(sems, pairs):
    copies = [pltpu.make_async_copy(src, dst, sems.at[i]) for i, (src, dst) in enumerate(pairs)]
    for copy in copies:
        copy.start()
    for copy in copies:
        copy.wait()


def layer_rows(weights, layer, count):
    rows = weights.shape[1] // count

    def kernel(weights_ref, *refs):
        source = weights_ref.at[layer]
        run_copies(
            refs[-1], [(source.at[pl.ds(i * rows, rows)], ref) for i, ref in enumerate(refs[:-1])]
        )

    return pl.pallas_call(
        kernel,
        out_shape=(pltpu.VMEM((rows, *weights.shape[2:]), weights.dtype),) * count,
        in_specs=[pl.BlockSpec(memory_space=pltpu.HBM)],
        out_specs=tuple(vmem_specs(count)),
        scratch_shapes=[pltpu.SemaphoreType.DMA((count,))],
        compiler_params=pltpu.CompilerParams(vmem_limit_bytes=KERNEL_VMEM),
        name="layer_rows",
    )(weights)


def weave_in(pieces, parts):
    width = pieces[0].shape[1]
    offsets = [sum(piece.shape[0] for piece in pieces[:i]) for i in range(len(pieces) + 1)]

    def kernel(*refs):
        pieces_refs, outs, sems = refs[: len(pieces)], refs[len(pieces) : -1], refs[-1]
        pairs = []
        for out_ref, (start, count) in zip(outs, parts):
            for i, piece in enumerate(pieces_refs):
                for side in range(2):
                    columns = pl.ds(side * (width // 2) + start, count)
                    place = out_ref.at[pl.ds(offsets[i], piece.shape[0]), pl.ds(side * count, count)]
                    pairs.append((piece.at[:, columns], place))
        run_copies(sems, pairs)

    return pl.pallas_call(
        kernel,
        out_shape=tuple(
            jax.ShapeDtypeStruct((offsets[-1], 2 * count), BF16) for _, count in parts
        ),
        in_specs=[pl.BlockSpec(memory_space=pltpu.HBM)] * len(pieces),
        out_specs=(pl.BlockSpec(memory_space=pltpu.HBM),) * len(parts),
        scratch_shapes=[pltpu.SemaphoreType.DMA((2 * len(parts) * len(pieces),))],
        compiler_params=pltpu.CompilerParams(vmem_limit_bytes=WOVEN_VMEM),
        name="weave_in",
    )(*pieces)


def weave_out(pieces):
    rows, width = pieces[0].shape
    low = rows // 2
    places = [(0, 0), (0, 1), (0, 2), (low, 2), (0, 3)]

    def kernel(*refs):
        out_ref, sems = refs[-2:]
        pairs = []
        for ref, piece, (row, column) in zip(refs, pieces, places):
            columns = pl.ds(column * width, width)
            pairs.append((ref, out_ref.at[pl.ds(row, piece.shape[0]), columns]))
        run_copies(sems, pairs)

    return pl.pallas_call(
        kernel,
        out_shape=pltpu.VMEM((rows, 4 * width), BF16),
        in_specs=[pl.BlockSpec(memory_space=pltpu.HBM)] * len(pieces),
        out_specs=vmem_specs(1)[0],
        scratch_shapes=[pltpu.SemaphoreType.DMA((len(pieces),))],
        compiler_params=pltpu.CompilerParams(vmem_limit_bytes=WOVEN_VMEM),
        name="weave_out",
    )(*pieces)


GROUPS = [
    [((y * 4 + z) * 4 + x) * 2 + c for y, z in members for x in range(4)]
    for c in range(2)
    for members in (
        [[(a, b) if c == 0 else (b, a) for a in range(4)] for b in range(4)]
    )
]


def exchange(blocks):
    flat = blocks.reshape(16, *blocks.shape[2:])
    flat = lax.all_to_all(
        flat, ("y", "z", "x", "c"), 0, 0, axis_index_groups=GROUPS, tiled=True
    )
    return flat.reshape(blocks.shape)


def gather_near(block):
    return block, across(block, 1), across(block, 3)


def relay_far(near):
    block, nearest, behind = near
    half = block.shape[0] // 2
    far_top, far_low = across(nearest[:half], 1), across(behind[half:], 3)
    return block, nearest, far_top, far_low, behind


def gather_weight(block):
    far = across(block, 2)
    return block, across(block, 1), far, across(block, 3)


def reduce_x(pieces):
    arrived = [fetch(pieces((-step) % 4), "x", step) for step in (2, 1, 3)]
    total = pieces(0).astype(F32)
    for piece in arrived:
        total = total + piece.astype(F32)
    return total.astype(BF16)


def per_device(
    patch_query,
    key_cache,
    value_cache,
    cache_len,
    patch_end,
    ended_index,
    pool_out,
    norm_gain,
    w_in,
    w_out,
):
    seq_rows, width = patch_query.shape
    heads_width = key_cache.shape[2]
    layers, _, _, hidden_local = w_in.shape
    y = lax.axis_index("y")
    z = lax.axis_index("z")
    x = lax.axis_index("x")
    c = lax.axis_index("c")
    quarter = width // 4

    own = jnp.where(c == 0, y, z)
    side = jnp.where(c == 0, z, y)
    position = jnp.arange(4, dtype=jnp.int32)
    first = position[:, None]
    second = (side + position[None, :]) % 4
    order = jnp.where(c == 0, first * 4 + second, second * 4 + first).reshape(16).astype(jnp.int32)
    large = hidden_local // 7 * 4
    parts = ((0, large), (large, hidden_local - large))

    def owned(product, step):
        return lax.dynamic_index_in_dim(product, (own + step) % 4, 0, keepdims=False)

    def weights_of(layer, w_in, w_out):
        rows = layer_rows(w_in, layer, 1)
        rows = [piece.reshape(-1, 2 * hidden_local) for piece in rows]
        gathered = gather_near(rows[0]) if layer else gather_weight(rows[0])
        return gathered, gather_near(w_out[layer])

    ins, outs = weights_of(0, w_in, w_out)

    slots = rotated(ended_index.reshape(4, 2, 16), x, 0)
    sequence = jnp.arange(seq_rows, dtype=jnp.int32)[None, :]
    own_picker = (slots[0].reshape(32, 1) == sequence).astype(BF16)
    picker = (rotated(slots, c, 1).reshape(128, 1) == sequence).astype(BF16)
    last_slots = rotated(slots, c, 1).transpose(1, 0, 2).reshape(128, 1)
    last_picker = (last_slots == sequence).astype(BF16)

    mp_index = x * 2 + c
    query_cols = lax.dynamic_slice_in_dim(patch_query, mp_index * heads_width, heads_width, 1)
    attended = attend_local(query_cols, key_cache, value_cache, cache_len)
    chosen = jnp.dot(picker, attended, preferred_element_type=F32).astype(BF16)
    partial = jnp.dot(chosen, pool_out, preferred_element_type=F32).astype(BF16)
    partial = partial.reshape(4, 2, 16, width)
    other = fetch(partial[:, 1], "c", 1)
    partial = (partial[:, 0].astype(F32) + other.astype(F32)).astype(BF16)
    mine = reduce_x(lambda r: partial[r])
    other = fetch(mine, "c", 1)
    first, second = jnp.where(c == 0, mine, other), jnp.where(c == 0, other, mine)
    mine = jnp.concatenate([first, second])
    other = jnp.zeros_like(mine)
    state = jnp.dot(own_picker, patch_query, preferred_element_type=F32)

    for layer in range(layers):
        state, blocks = add_and_norm(order, state, mine, other, norm_gain[layer])
        rows = exchange(blocks).reshape(4, 128, quarter)
        rows = rows.reshape(512, quarter)
        rows, ins = lax.optimization_barrier((rows, ins))
        halves = weave_in(ins, parts)
        products = []
        for part in range(2):
            products.append(jnp.dot(rows, halves[part], preferred_element_type=F32).astype(BF16))
        near, _ = lax.optimization_barrier((outs, products[1]))
        weight_out = weave_out(relay_far(near))
        if layer + 1 < layers:
            w_in, w_out, _ = lax.optimization_barrier((w_in, w_out, blocks))
            ins, outs = weights_of(layer + 1, w_in, w_out)
        partial = 0.0
        for part, (start, count) in enumerate(parts):
            product = products[part].reshape(4, 128, 2 * count)
            arrived = [along(owned(product, -s), s) for s in (2, 1, 3)]
            gate_up = owned(product, 0).astype(F32)
            for block in arrived:
                gate_up = gate_up + block.astype(F32)
            hidden = (jax.nn.silu(gate_up[:, :count]) * gate_up[:, count:]).astype(BF16)
            far = along(hidden, 2)
            all_hidden = jnp.concatenate([hidden, along(hidden, 1), far, along(hidden, 3)])
            partial = partial + jnp.dot(
                all_hidden, weight_out[start : start + count], preferred_element_type=F32
            )
        partial = rotated(partial.astype(BF16).reshape(4, 4, 32, quarter), (4 - own) % 4, 0)
        if layer + 1 < layers:
            ins = relay_far(ins)
        partial = exchange(partial)
        mine = summed_columns(order, partial)
        other = fetch(mine, "c", 1)

    update = mine.astype(F32) + other.astype(F32)
    state = (state + update.astype(BF16).astype(F32)).astype(BF16)
    piece = lax.dynamic_slice_in_dim(state, c * 16, 16, 0)
    far = fetch(piece, "x", 2)
    own_core = jnp.stack([piece, fetch(piece, "x", 1), far, fetch(piece, "x", 3)])
    whole = jnp.stack([own_core, fetch(own_core, "c", 1)]).reshape(128, width)
    placed = lax.dot_general(last_picker, whole, (((0,), (0,)), ((), ())), preferred_element_type=F32)
    return (placed * patch_end.astype(F32)[:, None]).astype(BF16)


def solution(mesh):
    torus = Mesh(mesh.devices.reshape(4, 4, 4, 2), ("y", "z", "x", "c"))
    dp, mp = ("y", "z"), ("x", "c")
    in_specs = (
        P(dp, None),
        P(dp, None, mp),
        P(dp, None, mp),
        P(dp),
        P(dp),
        P(dp),
        P(mp, None),
        P(),
        P(None, dp, None, mp),
        P(None, mp, dp),
    )
    return jax.shard_map(
        per_device, mesh=torus, in_specs=in_specs, out_specs=P(dp, None), check_vma=False
    )
```
